512 devices in a mesh: panel: 32 (over y_lo, z, core), rhs: 16 (over x, y_hi).
Axes of the slice: x: 4, y: 8 (y_hi: 4, y_lo: 2; y = y_hi * 2 + y_lo), z: 8, core: 2. Of those that a mesh axis runs over, the one named last changes fastest.
Arguments:
- pivot_rhs: float32 [2, 2048, 2048], P(None, 'panel', 'rhs'), may hold values from -6 to 6
- update_rhs: float32 [4096, 2048], P('panel', 'rhs'), may hold values from -6 to 6
- parent_rhs: float32 [4096, 2048], P('panel', 'rhs'), may hold values from -6 to 6
- lower_pivot: bfloat16 [2, 2048, 2048], P(None, 'panel', 'rhs'), may hold values from -1 to 1.4, as said below
- lower_update: bfloat16 [4096, 2048], P('panel', 'rhs'), may hold values from -0.125 to 0.125
- parent_lower: bfloat16 [4096, 4096], P('panel', 'rhs'), may hold values from -1 to 1.4, as said below
- parent_upper: bfloat16 [4096, 4096], P('panel', 'rhs'), may hold values from -1 to 1.4, as said below
- upper_pivot: bfloat16 [2, 2048, 2048], P(None, 'panel', 'rhs'), may hold values from -1 to 1.4, as said below
- upper_update: bfloat16 [2, 2048, 2048], P(None, 'panel', 'rhs'), may hold values from -0.125 to 0.125
- maps: int32 [4096], replicated, may hold values from 0 to 4095, as said below
Outputs:
- parent_solution: float32 [4096, 2048], P('panel', 'rhs')
- child_solution: float32 [2, 2048, 2048], P(None, 'panel', 'rhs')
The draws below stay inside these ranges and needn't reach their ends.
Inputs may be any that keep to these rules, and one draw needn't show every extreme that they name: `maps`: for each child k, entry k * 2048 + i is 2 * i + b with b equal to 0 or 1; both values of b occur for each child in every draw. `lower_pivot`: each block is lower triangular, diagonal 0.6 to 1.4. `upper_pivot`: each block is upper triangular, diagonal 0.6 to 1.4. `parent_lower`: lower triangular, diagonal 0.6 to 1.4. `parent_upper`: upper triangular, diagonal 0.6 to 1.4.
All inputs are finite; a program needn't handle non-finite values.
Results may differ from the reference program's by a relative error of at most 0.0054.
Values may be sent and summed in bfloat16 or wider, within the bound.
No kernel may reach another device: no remote copies, remote signals or barrier semaphores. Data moves between devices by JAX's collectives and lax.ppermute only.
A program may use at most 64 MiB of HBM per device.

```python
import math
import jax
import jax.numpy as jnp
from jax import lax

F = 4096
KC = 2048
FU = 2048
RHS = 2048


def triangle(random_key, block_count, matrix_order, lower_side):
    shape_full = (block_count, matrix_order, matrix_order)
    noise = jax.random.normal(random_key, shape_full, jnp.float32)
    noise = noise / math.sqrt(matrix_order)
    row_ids = lax.broadcasted_iota(jnp.int32, (matrix_order, matrix_order), 0)
    col_ids = lax.broadcasted_iota(jnp.int32, (matrix_order, matrix_order), 1)
    if lower_side:
        keeper = row_ids > col_ids
    else:
        keeper = row_ids < col_ids
    diagonal_scale = jax.random.uniform(jax.random.fold_in(random_key, 7), (block_count, matrix_order, 1), jnp.float32, 0.6, 1.4)
    identity = jnp.where(row_ids == col_ids, 1.0, 0.0).astype(jnp.float32)
    return jnp.where(keeper[None], noise, 0.0) + identity[None] * diagonal_scale


def draw_lower_pivot(key, part):
    return triangle(jax.random.fold_in(key, 101), 2, KC, True).astype(jnp.bfloat16)


def draw_upper_pivot(key, part):
    return triangle(jax.random.fold_in(key, 103), 2, KC, False).astype(jnp.bfloat16)


def draw_parent_lower(key, part):
    return triangle(jax.random.fold_in(key, 107), 1, F, True).reshape(F, F).astype(jnp.bfloat16)


def draw_parent_upper(key, part):
    return triangle(jax.random.fold_in(key, 109), 1, F, False).reshape(F, F).astype(jnp.bfloat16)


def draw_maps(key, part):
    local = lax.broadcasted_iota(jnp.int32, (FU,), 0)
    first_bits = jax.random.randint(jax.random.fold_in(key, 211), (FU,), 0, 2)
    first_bits = jnp.where(local == 0, 0, first_bits)
    first_bits = jnp.where(local == FU - 1, 1, first_bits)
    second_bits = jax.random.randint(jax.random.fold_in(key, 212), (FU,), 0, 2)
    second_bits = jnp.where(local == 0, 1, second_bits)
    second_bits = jnp.where(local == FU - 1, 0, second_bits)
    return jnp.concatenate([2 * local + first_bits, 2 * local + second_bits]).astype(jnp.int32)


def levels(key, dims, shards, smallest, top_value):
    factor_of, own = 1.0, jax.random.fold_in(key, 6)
    for axis_at, blocks in shards:
        draws = jnp.exp(jax.random.uniform(jax.random.fold_in(own, axis_at), (blocks,), jnp.float32, smallest / len(shards), top_value / len(shards)))
        factor_of = factor_of * jnp.repeat(draws, dims[axis_at] // blocks).reshape([-1 if axis == axis_at else 1 for axis in range(len(dims))])
    return factor_of


def normal_values(stream_key, extent, spread, bound, pieces=(), held_as=jnp.bfloat16):
    level = levels(stream_key, extent, pieces, -0.22, 0.18) if pieces else 1.0
    drawn = jax.random.normal(stream_key, extent, jnp.float32) * spread * level
    return jnp.minimum(jnp.maximum(drawn, -bound), bound).astype(held_as)


def setup_inputs(seed: int = 0) -> dict:
    key_of = jax.random.split(jax.random.key(seed), 11)
    return {
        "pivot_rhs": normal_values(key_of[0], (2, KC, RHS), 1.0, 6.0, ((1, 32), (2, 16)), jnp.float32),
        "update_rhs": normal_values(key_of[1], (2 * FU, RHS), 1.0, 6.0, ((0, 32), (1, 16)), jnp.float32),
        "parent_rhs": normal_values(key_of[2], (F, RHS), 1.0, 6.0, ((0, 32), (1, 16)), jnp.float32),
        "lower_pivot": draw_lower_pivot(jax.random.fold_in(key_of[10], 71), 0),
        "lower_update": normal_values(key_of[4], (2 * FU, KC), KC ** -0.5, 0.125, ((0, 32), (1, 16))),
        "parent_lower": draw_parent_lower(jax.random.fold_in(key_of[10], 71), 0),
        "parent_upper": draw_parent_upper(jax.random.fold_in(key_of[10], 71), 0),
        "upper_pivot": draw_upper_pivot(jax.random.fold_in(key_of[10], 71), 0),
        "upper_update": normal_values(key_of[8], (2, KC, FU), FU ** -0.5, 0.125, ((1, 32), (2, 16))),
        "maps": draw_maps(jax.random.fold_in(key_of[10], 71), 0),
    }


def product(left, right):
    return jnp.dot(left, right, preferred_element_type=jnp.float32)


def reference(pivot_rhs, update_rhs, parent_rhs, lower_pivot, lower_update, parent_lower, parent_upper, upper_pivot, upper_update, maps):
    pivot_input = pivot_rhs.astype(jnp.bfloat16)
    solved = []
    updates = []
    for member in range(2):
        source = pivot_input[member]
        solved.append(product(lower_pivot[member], source))
        updates.append(update_rhs[member * FU:(member + 1) * FU] + product(lower_update[member * FU:(member + 1) * FU], source))
    pivot_half = jnp.stack(solved, axis=0).astype(jnp.bfloat16)
    update_half = jnp.concatenate(updates, axis=0).astype(jnp.bfloat16)
    widened = lax.optimization_barrier(update_half).astype(jnp.float32)
    scattered = jnp.zeros(parent_rhs.shape, jnp.float32).at[maps].add(widened)
    parent_sum = parent_rhs + scattered
    parent_mid = product(parent_lower, parent_sum.astype(jnp.bfloat16))
    parent_solution = product(parent_upper, parent_mid.astype(jnp.bfloat16))
    solution_half = parent_solution.astype(jnp.bfloat16)
    blocks = []
    for member in range(2):
        picked = jnp.take(solution_half, maps[member * FU:(member + 1) * FU], axis=0)
        direct = product(upper_pivot[member], pivot_half[member])
        blocks.append(direct + product(upper_update[member], picked))
    return parent_solution, jnp.stack(blocks, axis=0)
```

```python
import functools

import jax
import jax.numpy as jnp
from jax import lax
from jax.experimental import pallas as pl
from jax.experimental.pallas import tpu as pltpu
from jax.sharding import Mesh, PartitionSpec as P

BF = jnp.bfloat16
F32 = jnp.float32
CHIPS = ("yl", "z")
RHS = ("x", "yh")
PANEL = ("yl", "z", "c")
NP = 16
W = 64
ROWS = 256
HALF = 128


def nt(a, b):
    return lax.dot_general(a, b, (((1,), (1,)), ((), ())), preferred_element_type=F32)


def nn(a, b):
    return lax.dot_general(a, b, (((1,), (0,)), ((), ())), preferred_element_type=F32)


def vmem():
    return pl.BlockSpec(memory_space=pltpu.VMEM)


def smem():
    return pl.BlockSpec(memory_space=pltpu.SMEM)


def call(kernel, outs, *args):
    return pl.pallas_call(
        kernel,
        out_shape=outs,
        in_specs=[smem()] + [vmem()] * (len(args) - 1),
        out_specs=jax.tree.map(lambda _: vmem(), outs),
    )(*args)


def ordered(both, core):
    half = both.shape[1] // 2
    swapped = jnp.concatenate([both[:, half:], both[:, :half]], axis=1)
    return jnp.where(core == 0, both, swapped)


def row_ids(core, n):
    at = lax.broadcasted_iota(jnp.int32, (n, n), 0)
    half = n // 2
    return jnp.where(core == 0, at, jnp.where(at < half, at + half, at - half))


def keep(x, cond):
    return jnp.where(cond, x, jnp.zeros_like(x))


def forward_children(pos, xg, fm, fo, ur, pr, e, send, ps_out, piv_out):
    chip, core = pos[0], pos[1]
    acc_m = jnp.zeros((W, HALF), F32)
    acc_o = jnp.zeros((W, HALF), F32)
    piv = [jnp.zeros((W, HALF), F32), jnp.zeros((W, HALF), F32)]
    for r in range(NP):
        x = xg[r]
        xs = (x[:, :HALF], x[:, HALF:])
        xc = jnp.where(core == 0, xs[0], xs[1])
        xo = jnp.where(core == 0, xs[1], xs[0])
        acc_m += nt(xc, fm[r, 0:HALF, :])
        acc_o += nt(xo, fo[r, 0:HALF, :])
        for k in range(2):
            lo = HALF + 64 * k
            block = jnp.concatenate([fm[r, lo : lo + 64, :], fo[r, lo : lo + 64, :]], axis=0)
            piv[k] += nt(keep(xs[k], r < chip), block)
    u0 = jnp.where(core == 0, acc_m, acc_o) + ur[0]
    u1 = jnp.where(core == 0, acc_o, acc_m) + ur[1]
    u = jnp.concatenate([u0.astype(BF), u1.astype(BF)], axis=1)
    ps = (pr[...] + nn(u, e[...])).astype(BF)
    rows = row_ids(core, HALF)
    cols = lax.broadcasted_iota(jnp.int32, (HALF, HALF), 1)
    own = xg[chip]
    outs = []
    for k in range(2):
        lo = HALF + 64 * k
        block = jnp.concatenate([fm[chip, lo : lo + 64, :], fo[chip, lo : lo + 64, :]], axis=0)
        x = own[:, k * HALF : (k + 1) * HALF]
        total = ordered(piv[k] + nt(x, keep(block, cols < rows)), core)
        diag = fm[chip, 256:272, :].astype(F32)[k : k + 1] + fo[chip, 256:272, :].astype(F32)[k : k + 1]
        outs.append((total + x.astype(F32) * diag).astype(BF))
    pivot = jnp.concatenate(outs, axis=1)
    ps_out[...] = ps
    piv_out[...] = pivot
    for q in range(NP):
        send[q] = jnp.where(chip <= q, ps, pivot)


def parent_forward(pos, g, ps_ref, mm, mo, send):
    chip, core = pos[0], pos[1]
    acc_m = jnp.zeros((W, HALF), F32)
    acc_o = jnp.zeros((W, HALF), F32)
    for r in range(NP):
        x = keep(g[r], r < chip)
        acc_m += nt(x, mm[r, 0:HALF, :])
        acc_o += nt(x, mo[r, 0:HALF, :])
    rows = row_ids(core, ROWS)
    cols = lax.broadcasted_iota(jnp.int32, (ROWS, ROWS), 1)
    block = jnp.concatenate([mm[chip, 0:HALF, :], mo[chip, 0:HALF, :]], axis=0)
    ps = ps_ref[...]
    total = ordered(jnp.concatenate([acc_m, acc_o], axis=1) + nt(ps, keep(block, cols < rows)), core)
    diag = mm[chip, 128:144, :].astype(F32)[0:1] + mo[chip, 128:144, :].astype(F32)[0:1]
    mid = (total + ps.astype(F32) * diag).astype(BF)
    for q in range(NP):
        send[q] = mid


def parent_backward(pos, g, mm, mo, e, send, sol_out):
    chip, core = pos[0], pos[1]
    acc_m = jnp.zeros((W, HALF), F32)
    acc_o = jnp.zeros((W, HALF), F32)
    for r in range(NP):
        x = keep(g[r], r > chip)
        acc_m += nt(x, mm[r, 0:HALF, :])
        acc_o += nt(x, mo[r, 0:HALF, :])
    rows = row_ids(core, ROWS)
    cols = lax.broadcasted_iota(jnp.int32, (ROWS, ROWS), 1)
    block = jnp.concatenate([mm[chip, 0:HALF, :], mo[chip, 0:HALF, :]], axis=0)
    sol = ordered(jnp.concatenate([acc_m, acc_o], axis=1) + nt(g[chip], keep(block, cols >= rows)), core)
    sol_out[...] = sol
    picked = nt(sol.astype(BF), e[...]).astype(BF)
    for q in range(NP):
        send[q] = picked


def pivot_backward(pos, g, piv_ref, fm, fo, out):
    chip, core = pos[0], pos[1]
    rows = row_ids(core, HALF)
    cols = lax.broadcasted_iota(jnp.int32, (HALF, HALF), 1)
    for k in range(2):
        lo = HALF + 64 * k
        acc = jnp.zeros((HALF, W), F32)
        for r in range(NP):
            block = jnp.concatenate([fm[r, lo : lo + 64, :], fo[r, lo : lo + 64, :]], axis=0)
            acc += nt(block, keep(g[r, :, k * HALF : (k + 1) * HALF], r > chip))
        block = jnp.concatenate([fm[chip, lo : lo + 64, :], fo[chip, lo : lo + 64, :]], axis=0)
        acc += nt(keep(block, cols >= rows), piv_ref[:, k * HALF : (k + 1) * HALF])
        out[k] = acc


def children_backward(pos, g, mm, mo, part, mine, other):
    for k in range(2):
        acc = part[k]
        for r in range(NP):
            cut = slice(k * HALF, (k + 1) * HALF)
            block = jnp.concatenate([mm[r, 144:208, cut], mo[r, 144:208, cut]], axis=0)
            acc += nt(block, g[r, :, cut])
        mine[k] = acc[:64]
        other[k] = acc[64:]


def to_all(block, axes, n):
    return lax.all_to_all(jnp.broadcast_to(block[None], (n, *block.shape)), axes, 0, 0, tiled=True)


def over_rhs(shard):
    by_y = to_all(shard, "yh", 4)
    by_x = to_all(by_y, "x", 4)
    return by_x.reshape(16, *shard.shape)


def partner(x):
    return lax.ppermute(x, "c", [(0, 1), (1, 0)])


def exchange(send):
    return lax.all_to_all(send, CHIPS, 0, 0, tiled=True)


def halves(x, core, axis):
    a, b = jnp.split(x, 2, axis=axis)
    return jnp.where(core == 0, a, b), jnp.where(core == 0, b, a)


def two_terms(x):
    high = lax.reduce_precision(x, 8, 7)
    return high.astype(BF), (x - high).astype(BF)


def shards(pivot_rhs, update_rhs, parent_rhs, lower_pivot, lower_update, parent_lower, parent_upper, upper_pivot, upper_update, maps):
    core = lax.axis_index("c")
    chip = lax.axis_index("yl") * 8 + lax.axis_index("z")
    group = lax.axis_index("x") * 4 + lax.axis_index("yh")
    pos = jnp.stack([chip, core]).astype(jnp.int32)

    to_parent = []
    for p in range(32):
        k, j = divmod(p, 16)
        to_parent.append((p, 2 * j + k))
    uh, ul = two_terms(update_rhs.T)
    moved = lax.ppermute(jnp.concatenate([lower_update, uh, ul], axis=0), PANEL, to_parent)

    xt = pivot_rhs.astype(BF).transpose(2, 0, 1).reshape(128, 128)
    ph, plo = two_terms(parent_rhs.T)
    x_mine, x_give = halves(xt, core, 0)
    ph_mine, ph_give = halves(ph, core, 0)
    pl_mine, pl_give = halves(plo, core, 0)
    got = partner(jnp.concatenate([x_give, ph_give, pl_give], axis=0))

    def sides(mine, other):
        return jnp.where(core == 0, mine, other), jnp.where(core == 0, other, mine)

    x0, x1 = sides(x_mine, got[:64])
    x_block = jnp.concatenate([x0[:, :64], x1[:, :64], x0[:, 64:], x1[:, 64:]], axis=1)
    pr_own = ph_mine.astype(F32) + pl_mine.astype(F32)
    pr_got = got[64:128].astype(F32) + got[128:].astype(F32)
    pr = jnp.concatenate(sides(pr_own, pr_got), axis=1)

    r_at = lax.broadcasted_iota(jnp.int32, (1, 64, 128), 1) + core * 64
    c_at = lax.broadcasted_iota(jnp.int32, (1, 64, 128), 2)
    full_l, on_block = group < chip, group == chip
    pick_low = jnp.logical_or(full_l, jnp.logical_and(on_block, c_at < r_at))
    pivots = jnp.where(pick_low, lower_pivot, upper_pivot).reshape(128, 128)
    diag = jnp.sum(jnp.where(jnp.logical_and(on_block, c_at == r_at), lower_pivot, jnp.zeros_like(lower_pivot)), axis=1)
    diag = jnp.pad(diag, ((0, 14), (0, 0)))
    first = over_rhs(jnp.concatenate([moved[:128], pivots, diag], axis=0))
    first_other = partner(first)

    xg = to_all(x_block, CHIPS, NP)

    r_at = lax.broadcasted_iota(jnp.int32, (128, 256), 0) + core * 128
    c_at = lax.broadcasted_iota(jnp.int32, (128, 256), 1)
    pick_low = jnp.logical_or(full_l, jnp.logical_and(on_block, c_at < r_at))
    parents = jnp.where(pick_low, parent_lower, parent_upper)
    pdiag = jnp.sum(jnp.where(jnp.logical_and(on_block, c_at == r_at), parent_lower, jnp.zeros_like(parent_lower)), axis=0)
    pdiag = jnp.pad(pdiag[None], ((0, 15), (0, 0)))
    uu = jnp.concatenate([upper_update[0], upper_update[1]], axis=1)
    second = over_rhs(jnp.concatenate([parents, pdiag, uu], axis=0))
    second_other = partner(second)

    uh_mine, uh_give = halves(moved[128:256], core, 0)
    ul_mine, ul_give = halves(moved[256:384], core, 0)
    got = partner(jnp.concatenate([uh_give, ul_give], axis=0))
    ur_own = uh_mine.astype(F32) + ul_mine.astype(F32)
    ur_got = got[:64].astype(F32) + got[64:].astype(F32)
    ur = jnp.stack(sides(ur_own, ur_got), axis=0)

    own_maps = lax.dynamic_slice(maps.reshape(2, 2048), (0, chip * 128), (2, 128)).reshape(256, 1)
    spots = lax.broadcasted_iota(jnp.int32, (256, 256), 1) + chip * 256
    e = (own_maps == spots).astype(BF)

    block = jax.ShapeDtypeStruct((W, ROWS), BF)
    sent = jax.ShapeDtypeStruct((NP, W, ROWS), BF)
    send2, ps, piv = call(forward_children, [sent, block, block], pos, xg, first, first_other, ur, pr, e)
    g2 = exchange(send2)
    send3 = call(parent_forward, sent, pos, g2, ps, second, second_other)
    g3 = exchange(send3)
    part = call(pivot_backward, jax.ShapeDtypeStruct((2, HALF, W), F32), pos, g2, piv, first, first_other)
    send4, sol_t = call(parent_backward, [sent, jax.ShapeDtypeStruct((W, ROWS), F32)], pos, g3, second, second_other, e)
    g4 = exchange(send4)

    s0, s1 = halves(sol_t, core, 1)
    s_got = partner(s1)
    parent_solution = jnp.concatenate(sides(s0, s_got), axis=0).T

    out_half = jax.ShapeDtypeStruct((2, 64, W), F32)
    mine, other = call(children_backward, [out_half, out_half], pos, g4, second, second_other, part)
    got = partner(other)
    child_solution = jnp.concatenate(sides(mine, got), axis=2)
    return (parent_solution, child_solution)


def solution(mesh):
    fine = Mesh(mesh.devices.reshape(2, 8, 2, 4, 4), ("yl", "z", "c", "x", "yh"))
    three = P(None, PANEL, RHS)
    two = P(PANEL, RHS)
    return jax.shard_map(
        shards,
        mesh=fine,
        in_specs=(three, two, two, three, two, two, two, three, three, P()),
        out_specs=(two, three),
        check_vma=False,
    )
```

```python
import jax
import jax.numpy as jnp
from jax import lax
from jax.experimental import pallas as pl
from jax.experimental.pallas import tpu as pltpu
from jax.sharding import Mesh, PartitionSpec as P


BF = jnp.bfloat16
F32 = jnp.float32
CHIPS = ("yl", "z")
RHS = ("x", "yh")
PANEL = ("yl", "z", "c")
NP = 16
W = 64
ROWS = 256
HALF = 128


def nt(a, b):
    return lax.dot_general(a, b, (((1,), (1,)), ((), ())), preferred_element_type=F32)


def nn(a, b):
    return lax.dot_general(a, b, (((1,), (0,)), ((), ())), preferred_element_type=F32)


def vmem():
    return pl.BlockSpec(memory_space=pltpu.VMEM)


def smem():
    return pl.BlockSpec(memory_space=pltpu.SMEM)


def near(x):
    return pltpu.with_memory_space_constraint(x, pltpu.VMEM)


def call(kernel, outs, pos, *args):
    args = [pos] + [near(a) if a.ndim > 2 else a for a in args]
    return pl.pallas_call(
        kernel,
        out_shape=outs,
        in_specs=[smem()] + [vmem()] * (len(args) - 1),
        out_specs=jax.tree.map(lambda _: vmem(), outs),
        compiler_params=pltpu.CompilerParams(vmem_limit_bytes=16 * 2**20),
    )(*args)


def ordered(both, core):
    half = both.shape[1] // 2
    swapped = jnp.concatenate([both[:, half:], both[:, :half]], axis=1)
    return jnp.where(core == 0, both, swapped)


def row_ids(core, n):
    at = lax.broadcasted_iota(jnp.int32, (n, n), 0)
    half = n // 2
    return jnp.where(core == 0, at, jnp.where(at < half, at + half, at - half))


def keep(x, cond):
    return jnp.where(cond, x, jnp.zeros_like(x))


def pivot_rows(mine, other, at, k):
    cut = slice(k * HALF, (k + 1) * HALF)
    return jnp.concatenate([mine[at, 64:128, cut], other[at, 64:128, cut]], axis=0)


def update_rows(f, at):
    return jnp.concatenate([f[at, 0:64, :HALF], f[at, 0:64, HALF:]], axis=0)


def forward_children(pos, xg, fm, fo, ur, pr, e, send, ps_out, piv_out):
    chip, core, mid_at = pos[0], pos[1], pos[2]
    acc_m = jnp.zeros((W, HALF), F32)
    acc_o = jnp.zeros((W, HALF), F32)
    piv = [jnp.zeros((W, HALF), F32), jnp.zeros((W, HALF), F32)]
    for r in range(NP):
        src = pos[4 + r]
        x = xg[src]
        xs = (x[:, :HALF], x[:, HALF:])
        xc = jnp.where(core == 0, xs[0], xs[1])
        xo = jnp.where(core == 0, xs[1], xs[0])
        acc_m += nt(xc, update_rows(fm, r))
        acc_o += nt(xo, update_rows(fo, r))
        for k in range(2):
            piv[k] += nt(keep(xs[k], src < chip), pivot_rows(fm, fo, r, k))
    u0 = jnp.where(core == 0, acc_m, acc_o) + ur[0]
    u1 = jnp.where(core == 0, acc_o, acc_m) + ur[1]
    u = jnp.concatenate([u0.astype(BF), u1.astype(BF)], axis=1)
    ps = (pr[...] + nn(u, e[...])).astype(BF)
    rows = row_ids(core, HALF)
    cols = lax.broadcasted_iota(jnp.int32, (HALF, HALF), 1)
    own = xg[chip]
    diag = fm[mid_at, 128:144, :].astype(F32)[0:1] + fo[mid_at, 128:144, :].astype(F32)[0:1]
    outs = []
    for k in range(2):
        cut = slice(k * HALF, (k + 1) * HALF)
        x = own[:, cut]
        total = ordered(piv[k] + nt(x, keep(pivot_rows(fm, fo, mid_at, k), cols < rows)), core)
        outs.append((total + x.astype(F32) * diag[:, cut]).astype(BF))
    pivot = jnp.concatenate(outs, axis=1)
    ps_out[...] = ps
    piv_out[...] = pivot
    for q in range(NP):
        send[q] = jnp.where(chip <= q, ps, pivot)


def parent_forward(pos, g, ps_ref, mm, mo, send):
    chip, core, mid_at = pos[0], pos[1], pos[3]
    acc_m = jnp.zeros((W, HALF), F32)
    acc_o = jnp.zeros((W, HALF), F32)
    for r in range(NP):
        src = pos[20 + r]
        x = keep(g[src], src < chip)
        acc_m += nt(x, mm[r, 0:HALF, :])
        acc_o += nt(x, mo[r, 0:HALF, :])
    rows = row_ids(core, ROWS)
    cols = lax.broadcasted_iota(jnp.int32, (ROWS, ROWS), 1)
    block = jnp.concatenate([mm[mid_at, 0:HALF, :], mo[mid_at, 0:HALF, :]], axis=0)
    ps = ps_ref[...]
    total = ordered(jnp.concatenate([acc_m, acc_o], axis=1) + nt(ps, keep(block, cols < rows)), core)
    diag = mm[mid_at, 128:144, :].astype(F32)[0:1] + mo[mid_at, 128:144, :].astype(F32)[0:1]
    mid = (total + ps.astype(F32) * diag).astype(BF)
    for q in range(NP):
        send[q] = mid


def parent_backward(pos, g, mm, mo, e, send, sol_out):
    chip, core, mid_at = pos[0], pos[1], pos[3]
    acc_m = jnp.zeros((W, HALF), F32)
    acc_o = jnp.zeros((W, HALF), F32)
    for r in range(NP):
        src = pos[20 + r]
        x = keep(g[src], src > chip)
        acc_m += nt(x, mm[r, 0:HALF, :])
        acc_o += nt(x, mo[r, 0:HALF, :])
    rows = row_ids(core, ROWS)
    cols = lax.broadcasted_iota(jnp.int32, (ROWS, ROWS), 1)
    block = jnp.concatenate([mm[mid_at, 0:HALF, :], mo[mid_at, 0:HALF, :]], axis=0)
    sol = ordered(jnp.concatenate([acc_m, acc_o], axis=1) + nt(g[chip], keep(block, cols >= rows)), core)
    sol_out[...] = sol
    picked = nt(sol.astype(BF), e[...]).astype(BF)
    for q in range(NP):
        send[q] = picked


def pivot_backward(pos, g, piv_ref, fm, fo, out):
    chip, core, mid_at = pos[0], pos[1], pos[2]
    rows = row_ids(core, HALF)
    cols = lax.broadcasted_iota(jnp.int32, (HALF, HALF), 1)
    for k in range(2):
        cut = slice(k * HALF, (k + 1) * HALF)
        acc = jnp.zeros((HALF, W), F32)
        for r in range(NP):
            src = pos[4 + r]
            acc += nt(pivot_rows(fm, fo, r, k), keep(g[src, :, cut], src > chip))
        acc += nt(keep(pivot_rows(fm, fo, mid_at, k), cols >= rows), piv_ref[:, cut])
        out[k] = acc


def children_backward(pos, g, um, uo, part, mine, other):
    for k in range(2):
        acc = part[k]
        for r in range(NP):
            cut = slice(k * HALF, (k + 1) * HALF)
            block = jnp.concatenate([um[r, :, cut], uo[r, :, cut]], axis=0)
            acc += nt(block, g[pos[20 + r], :, cut])
        mine[k] = acc[:64]
        other[k] = acc[64:]


def to_all(block, axes, n):
    return lax.all_to_all(jnp.broadcast_to(block[None], (n, *block.shape)), axes, 0, 0, tiled=True)


def shifts(x, axis):
    return [x] + [lax.ppermute(x, axis, [(i, (i + k) % 4) for i in range(4)]) for k in (1, 2, 3)]


def partner(x):
    return lax.ppermute(x, "c", [(0, 1), (1, 0)])


def after(x, *done):
    return lax.optimization_barrier((x, done))[0]


def exchange(send):
    return lax.all_to_all(send, CHIPS, 0, 0, tiled=True)


def halves(x, core, axis):
    a, b = jnp.split(x, 2, axis=axis)
    return jnp.where(core == 0, a, b), jnp.where(core == 0, b, a)


def two_terms(x):
    high = lax.reduce_precision(x, 8, 7)
    return high.astype(BF), (x - high).astype(BF)


def shards(pivot_rhs, update_rhs, parent_rhs, lower_pivot, lower_update, parent_lower, parent_upper, upper_pivot, upper_update, maps):
    core = lax.axis_index("c")
    chip = lax.axis_index("yl") * 8 + lax.axis_index("z")
    group = lax.axis_index("x") * 4 + lax.axis_index("yh")
    place = jnp.arange(4)
    gx, gy = lax.axis_index("x"), lax.axis_index("yh")
    y_from = (gy - place) % 4
    x_from = (gx - place) % 4
    y_at = (gy - chip % 4) % 4
    sources_ax = (place[:, None] * 4 + y_from[None, :]).reshape(16)
    sources_rx = (x_from[:, None] * 4 + y_from[None, :]).reshape(16)
    mid_ax = chip // 4 * 4 + y_at
    mid_rx = (gx - chip // 4) % 4 * 4 + y_at
    pos = jnp.concatenate([jnp.stack([chip, core, mid_ax, mid_rx]), sources_ax, sources_rx]).astype(jnp.int32)

    to_parent = []
    for p in range(32):
        k, j = divmod(p, 16)
        to_parent.append((p, 2 * j + k))
    uh, ul = two_terms(update_rhs.T)
    moved = lax.ppermute(jnp.concatenate([lower_update, uh, ul], axis=0), PANEL, to_parent)

    xt = pivot_rhs.astype(BF).transpose(2, 0, 1).reshape(128, 128)
    ph, plo = two_terms(parent_rhs.T)
    x_mine, x_give = halves(xt, core, 0)
    ph_mine, ph_give = halves(ph, core, 0)
    pl_mine, pl_give = halves(plo, core, 0)
    got = partner(jnp.concatenate([x_give, ph_give, pl_give], axis=0))

    def sides(mine, other):
        return jnp.where(core == 0, mine, other), jnp.where(core == 0, other, mine)

    x0, x1 = sides(x_mine, got[:64])
    x_block = jnp.concatenate([x0[:, :64], x1[:, :64], x0[:, 64:], x1[:, 64:]], axis=1)
    pr_own = ph_mine.astype(F32) + pl_mine.astype(F32)
    pr_got = got[64:128].astype(F32) + got[128:].astype(F32)
    pr = jnp.concatenate(sides(pr_own, pr_got), axis=1)

    xg = to_all(x_block, CHIPS, NP)

    full_l, on_block = group < chip, group == chip
    r_at = lax.broadcasted_iota(jnp.int32, (1, 64, 128), 1) + core * 64
    c_at = lax.broadcasted_iota(jnp.int32, (1, 64, 128), 2)
    pick_low = jnp.logical_or(full_l, jnp.logical_and(on_block, c_at < r_at))
    pivots = jnp.where(pick_low, lower_pivot, upper_pivot)
    diag = jnp.sum(jnp.where(jnp.logical_and(on_block, c_at == r_at), lower_pivot, jnp.zeros_like(lower_pivot)), axis=1)
    r_at = lax.broadcasted_iota(jnp.int32, (128, 256), 0) + core * 128
    c_at = lax.broadcasted_iota(jnp.int32, (128, 256), 1)
    pick_low = jnp.logical_or(full_l, jnp.logical_and(on_block, c_at < r_at))
    parents = jnp.where(pick_low, parent_lower, parent_upper)
    pdiag = jnp.sum(jnp.where(jnp.logical_and(on_block, c_at == r_at), parent_lower, jnp.zeros_like(parent_lower)), axis=0)
    diags = jnp.stack([jnp.concatenate([diag[0], diag[1]]), pdiag])
    diags = jnp.broadcast_to(diags[:, None], (2, 16, 256))

    def side_by_side(two):
        return jnp.concatenate([two[0], two[1]], axis=1)

    own = jnp.concatenate(
        [side_by_side((moved[0:64], moved[64:128])), side_by_side(pivots), diags[0], parents, diags[1]], axis=0
    )
    by_y = shifts(own, "yh")
    first_y, xg = lax.optimization_barrier((jnp.stack([a[:144] for a in by_y]), xg))
    first = to_all(first_y, "x", 4).reshape(16, 144, 256)
    first_other = partner(first)
    second_y = jnp.stack([a[144:] for a in by_y])
    second_x = shifts(second_y, "x")

    uh_mine, uh_give = halves(moved[128:256], core, 0)
    ul_mine, ul_give = halves(moved[256:384], core, 0)
    got = partner(jnp.concatenate([uh_give, ul_give], axis=0))
    ur_own = uh_mine.astype(F32) + ul_mine.astype(F32)
    ur_got = got[:64].astype(F32) + got[64:].astype(F32)
    ur = jnp.stack(sides(ur_own, ur_got), axis=0)

    own_maps = lax.dynamic_slice(maps.reshape(2, 2048), (0, chip * 128), (2, 128)).reshape(256, 1)
    spots = lax.broadcasted_iota(jnp.int32, (256, 256), 1) + chip * 256
    e = (own_maps == spots).astype(BF)

    block = jax.ShapeDtypeStruct((W, ROWS), BF)
    sent = jax.ShapeDtypeStruct((NP, W, ROWS), BF)
    send2, ps, piv = call(forward_children, [sent, block, block], pos, xg, first, first_other, ur, pr, e)
    g2 = exchange(send2)
    second = jnp.concatenate(after(second_x, ps), axis=0)
    second_other = partner(second)
    last_y = jnp.stack(shifts(after(side_by_side(upper_update), ps), "yh"))
    send3 = call(parent_forward, sent, pos, g2, ps, second, second_other)
    g3 = exchange(send3)
    last_x = shifts(after(last_y, send3), "x")
    part = call(pivot_backward, jax.ShapeDtypeStruct((2, HALF, W), F32), pos, g2, piv, first, first_other)
    send4, sol_t = call(parent_backward, [sent, jax.ShapeDtypeStruct((W, ROWS), F32)], pos, g3, second, second_other, e)
    g4 = exchange(send4)
    last = jnp.concatenate(after(last_x, sol_t), axis=0)
    last_other = partner(last)

    s0, s1 = halves(sol_t, core, 1)
    s_got = partner(s1)
    parent_solution = jnp.concatenate(sides(s0, s_got), axis=0).T

    out_half = jax.ShapeDtypeStruct((2, 64, W), F32)
    mine, other = call(children_backward, [out_half, out_half], pos, g4, last, last_other, part)
    got = partner(other)
    child_solution = jnp.concatenate(sides(mine, got), axis=2)
    return (parent_solution, child_solution)


def solution(mesh):
    fine = Mesh(mesh.devices.reshape(2, 8, 2, 4, 4), ("yl", "z", "c", "x", "yh"))
    three = P(None, PANEL, RHS)
    two = P(PANEL, RHS)

    return jax.shard_map(
        shards,
        mesh=fine,
        in_specs=(three, two, two, three, two, two, two, three, three, P()),
        out_specs=(two, three),
        check_vma=False,
    )
```

```python
import jax
import jax.numpy as jnp
from jax import lax
from jax.experimental import pallas as pl
from jax.experimental.pallas import tpu as pltpu
from jax.sharding import Mesh, PartitionSpec as P


BF = jnp.bfloat16
F32 = jnp.float32
CHIPS = ("yl", "z")
RHS = ("x", "yh")
PANEL = ("yl", "z", "c")
NP = 16
W = 64
ROWS = 256
HALF = 128


def nt(a, b):
    return lax.dot_general(a, b, (((1,), (1,)), ((), ())), preferred_element_type=F32)


def nn(a, b):
    return lax.dot_general(a, b, (((1,), (0,)), ((), ())), preferred_element_type=F32)


def vmem():
    return pl.BlockSpec(memory_space=pltpu.VMEM)


def smem():
    return pl.BlockSpec(memory_space=pltpu.SMEM)


def near(x):
    return pltpu.with_memory_space_constraint(x, pltpu.VMEM)


def call(kernel, outs, pos, *args):
    args = [pos] + [near(a) if a.ndim > 2 else a for a in args]
    return pl.pallas_call(
        kernel,
        out_shape=outs,
        in_specs=[smem()] + [vmem()] * (len(args) - 1),
        out_specs=jax.tree.map(lambda _: vmem(), outs),
        compiler_params=pltpu.CompilerParams(vmem_limit_bytes=16 * 2**20),
    )(*args)


def ordered(both, core):
    half = both.shape[1] // 2
    swapped = jnp.concatenate([both[:, half:], both[:, :half]], axis=1)
    return jnp.where(core == 0, both, swapped)


def row_ids(core, n):
    at = lax.broadcasted_iota(jnp.int32, (n, n), 0)
    half = n // 2
    return jnp.where(core == 0, at, jnp.where(at < half, at + half, at - half))


def keep(x, cond):
    return jnp.where(cond, x, jnp.zeros_like(x))


def pivot_rows(mine, other, at, k):
    cut = slice(k * HALF, (k + 1) * HALF)
    return jnp.concatenate([mine[at, 64:128, cut], other[at, 64:128, cut]], axis=0)


def update_rows(f, at):
    return jnp.concatenate([f[at, 0:64, :HALF], f[at, 0:64, HALF:]], axis=0)


def own_columns(core, rows):
    turned = rows.T
    return jnp.where(core == 0, turned[:W], turned[W:])


def first_block(pos, mine, other, send):
    core = pos[1]
    a = mine[...].astype(F32)
    b = other[...].astype(F32)
    low, high = jnp.where(core == 0, a, b), jnp.where(core == 0, b, a)
    rows = jnp.concatenate([low[:64], high[:64], low[64:], high[64:]], axis=0)
    block = own_columns(core, rows).astype(BF)
    for q in range(NP):
        send[q] = block


def join(pos, a, b, c, d, out):
    for i, x in enumerate((a, b, c, d)):
        out[4 * i : 4 * i + 4] = x[...]


def joined(pos, pieces):
    n, *rest = pieces[0].shape
    return call(join, jax.ShapeDtypeStruct((4 * n, *rest), pieces[0].dtype), pos, *pieces)


def forward_children(pos, xg, fm, fo, mine, other, e, send, piv_out, diag_out):
    chip, core, mid_at = pos[0], pos[1], pos[2]
    acc_m = jnp.zeros((W, HALF), F32)
    acc_o = jnp.zeros((W, HALF), F32)
    piv = [jnp.zeros((W, HALF), F32), jnp.zeros((W, HALF), F32)]
    for r in range(NP):
        src = pos[4 + r]
        x = xg[src]
        xs = (x[:, :HALF], x[:, HALF:])
        xc = jnp.where(core == 0, xs[0], xs[1])
        xo = jnp.where(core == 0, xs[1], xs[0])
        acc_m += nt(xc, update_rows(fm, r))
        acc_o += nt(xo, update_rows(fo, r))
        for k in range(2):
            piv[k] += nt(keep(xs[k], src < chip), pivot_rows(fm, fo, r, k))
    terms = [x[...].astype(F32) for x in (mine, other)]
    acc_m += own_columns(core, terms[0][:HALF] + terms[0][HALF : 2 * HALF])
    acc_o += own_columns(core, terms[1][:HALF] + terms[1][HALF : 2 * HALF])
    u0 = jnp.where(core == 0, acc_m, acc_o)
    u1 = jnp.where(core == 0, acc_o, acc_m)
    pr_m, pr_o = (t[2 * HALF : 3 * HALF] + t[3 * HALF :] for t in terms)
    pr_rows = jnp.concatenate([jnp.where(core == 0, pr_m, pr_o), jnp.where(core == 0, pr_o, pr_m)], axis=0)
    pr = own_columns(core, pr_rows)
    u = jnp.concatenate([u0.astype(BF), u1.astype(BF)], axis=1)
    ps = (pr + nn(u, e[...])).astype(BF)
    rows = row_ids(core, HALF)
    cols = lax.broadcasted_iota(jnp.int32, (HALF, HALF), 1)
    own = xg[chip]
    diag = fm[mid_at, 128:144, :].astype(F32)[0:1] + fo[mid_at, 128:144, :].astype(F32)[0:1]
    outs = []
    for k in range(2):
        cut = slice(k * HALF, (k + 1) * HALF)
        x = own[:, cut]
        total = ordered(piv[k] + nt(x, keep(pivot_rows(fm, fo, mid_at, k), cols < rows)), core)
        outs.append((total + x.astype(F32) * diag[:, cut]).astype(BF))
    pivot = jnp.concatenate(outs, axis=1)
    piv_out[...] = pivot
    diag_out[0] = fm[mid_at, 128:144, :]
    diag_out[1] = fo[mid_at, 128:144, :]
    for q in range(NP):
        send[q] = jnp.where(chip <= q, ps, pivot)


def parent_forward(pos, g, mm, mo, diags, send):
    chip, core, mid_at = pos[0], pos[1], pos[3]
    acc_m = jnp.zeros((W, HALF), F32)
    acc_o = jnp.zeros((W, HALF), F32)
    for r in range(NP):
        src = pos[20 + r]
        x = keep(g[src], src < chip)
        acc_m += nt(x, mm[r, 0:HALF, :])
        acc_o += nt(x, mo[r, 0:HALF, :])
    rows = row_ids(core, ROWS)
    cols = lax.broadcasted_iota(jnp.int32, (ROWS, ROWS), 1)
    block = jnp.concatenate([mm[mid_at, 0:HALF, :], mo[mid_at, 0:HALF, :]], axis=0)
    ps = g[chip]
    total = ordered(jnp.concatenate([acc_m, acc_o], axis=1) + nt(ps, keep(block, cols < rows)), core)
    diag = diags[0].astype(F32)[1:2] + diags[1].astype(F32)[1:2]
    mid = (total + ps.astype(F32) * diag).astype(BF)
    for q in range(NP):
        send[q] = mid


def parent_backward(pos, g, mm, mo, e, send, sol_out):
    chip, core, mid_at = pos[0], pos[1], pos[3]
    acc_m = jnp.zeros((W, HALF), F32)
    acc_o = jnp.zeros((W, HALF), F32)
    for r in range(NP):
        src = pos[20 + r]
        x = keep(g[src], src > chip)
        acc_m += nt(x, mm[r, 0:HALF, :])
        acc_o += nt(x, mo[r, 0:HALF, :])
    rows = row_ids(core, ROWS)
    cols = lax.broadcasted_iota(jnp.int32, (ROWS, ROWS), 1)
    block = jnp.concatenate([mm[mid_at, 0:HALF, :], mo[mid_at, 0:HALF, :]], axis=0)
    sol = ordered(jnp.concatenate([acc_m, acc_o], axis=1) + nt(g[chip], keep(block, cols >= rows)), core)
    sol_out[...] = sol
    picked = nt(sol.astype(BF), e[...]).astype(BF)
    for q in range(NP):
        send[q] = picked


def pivot_backward(pos, g, piv_ref, fm, fo, out):
    chip, core, mid_at = pos[0], pos[1], pos[2]
    rows = row_ids(core, HALF)
    cols = lax.broadcasted_iota(jnp.int32, (HALF, HALF), 1)
    for k in range(2):
        cut = slice(k * HALF, (k + 1) * HALF)
        acc = jnp.zeros((HALF, W), F32)
        for r in range(NP):
            src = pos[4 + r]
            acc += nt(pivot_rows(fm, fo, r, k), keep(g[src, :, cut], src > chip))
        acc += nt(keep(pivot_rows(fm, fo, mid_at, k), cols >= rows), piv_ref[:, cut])
        out[k] = acc


def children_backward(pos, g, um, uo, part, mine, other):
    for k in range(2):
        acc = part[k]
        for r in range(NP):
            cut = slice(k * HALF, (k + 1) * HALF)
            block = jnp.concatenate([um[r, 128:192, cut], uo[r, 128:192, cut]], axis=0)
            acc += nt(block, g[pos[20 + r], :, cut])
        mine[k] = acc[:64]
        other[k] = acc[64:]


def to_all(block, axes, n):
    return lax.all_to_all(jnp.broadcast_to(block[None], (n, *block.shape)), axes, 0, 0, tiled=True)


def shifts(x, axis):
    moved = [x]
    for k in (1, 2, 3):
        moved.append(lax.ppermute(x, axis, [(i, (i + k) % 4) for i in range(4)]))
    return moved


def partner(x):
    return lax.ppermute(x, "c", [(0, 1), (1, 0)])


def after(x, *done):
    return lax.optimization_barrier((x, done))[0]


def exchange(send):
    return lax.all_to_all(send, CHIPS, 0, 0, tiled=True)


def halves(x, core, axis):
    a, b = jnp.split(x, 2, axis=axis)
    return jnp.where(core == 0, a, b), jnp.where(core == 0, b, a)


def two_terms(x):
    high = lax.reduce_precision(x, 8, 7)
    return high.astype(BF), (x - high).astype(BF)


def shards(pivot_rhs, update_rhs, parent_rhs, lower_pivot, lower_update, parent_lower, parent_upper, upper_pivot, upper_update, maps):
    core = lax.axis_index("c")
    chip = lax.axis_index("yl") * 8 + lax.axis_index("z")
    group = lax.axis_index("x") * 4 + lax.axis_index("yh")
    place = jnp.arange(4)
    gx, gy = lax.axis_index("x"), lax.axis_index("yh")
    y_from = (gy - place) % 4
    x_from = (gx - place) % 4
    y_at = (gy - chip % 4) % 4
    sources_ax = (place[:, None] * 4 + y_from[None, :]).reshape(16)
    sources_rx = (x_from[:, None] * 4 + y_from[None, :]).reshape(16)
    mid_ax = chip // 4 * 4 + y_at
    mid_rx = (gx - chip // 4) % 4 * 4 + y_at
    pos = jnp.concatenate([jnp.stack([chip, core, mid_ax, mid_rx]), sources_ax, sources_rx]).astype(jnp.int32)

    to_parent = []
    for p in range(32):
        k, j = divmod(p, 16)
        to_parent.append((p, 2 * j + k))
    uh, ul = two_terms(update_rhs)
    moved = lax.ppermute(jnp.concatenate([lower_update, uh, ul], axis=0), PANEL, to_parent)

    x_rows = pivot_rhs.astype(BF).reshape(128, 128)
    x_other = partner(x_rows)
    sent = jax.ShapeDtypeStruct((NP, W, ROWS), BF)
    send1 = call(first_block, sent, pos, x_rows, x_other)
    xg = exchange(send1)

    def sides(mine, other):
        return jnp.where(core == 0, mine, other), jnp.where(core == 0, other, mine)

    full_l, on_block = group < chip, group == chip
    r_at = lax.broadcasted_iota(jnp.int32, (1, 64, 128), 1) + core * 64
    c_at = lax.broadcasted_iota(jnp.int32, (1, 64, 128), 2)
    pick_low = jnp.logical_or(full_l, jnp.logical_and(on_block, c_at < r_at))
    pivots = jnp.where(pick_low, lower_pivot, upper_pivot)
    diag = jnp.sum(jnp.where(jnp.logical_and(on_block, c_at == r_at), lower_pivot, jnp.zeros_like(lower_pivot)), axis=1)
    r_at = lax.broadcasted_iota(jnp.int32, (128, 256), 0) + core * 128
    c_at = lax.broadcasted_iota(jnp.int32, (128, 256), 1)
    pick_low = jnp.logical_or(full_l, jnp.logical_and(on_block, c_at < r_at))
    parents = jnp.where(pick_low, parent_lower, parent_upper)
    pdiag = jnp.sum(jnp.where(jnp.logical_and(on_block, c_at == r_at), parent_lower, jnp.zeros_like(parent_lower)), axis=0)
    diags = jnp.pad(jnp.stack([jnp.concatenate([diag[0], diag[1]]), pdiag]), ((0, 14), (0, 0)))

    def side_by_side(two):
        return jnp.concatenate([two[0], two[1]], axis=1)

    first_own = jnp.concatenate([side_by_side((moved[0:64], moved[64:128])), side_by_side(pivots), diags], axis=0)
    second_own = jnp.concatenate([parents, side_by_side(upper_update)], axis=0)
    first_y = shifts(first_own, "yh")
    first_y, xg = lax.optimization_barrier((jnp.stack(first_y), xg))
    first = to_all(first_y, "x", 4).reshape(16, 144, 256)
    first_other = partner(first)
    second_y = jnp.stack(shifts(after(second_own, first_y), "yh"))
    second_x = shifts(second_y, "x")

    ph, plo = two_terms(parent_rhs)
    others = jnp.concatenate([moved[128:], ph, plo], axis=0)
    others_got = partner(others)

    own_maps = lax.dynamic_slice(maps.reshape(2, 2048), (0, chip * 128), (2, 128)).reshape(256, 1)
    spots = lax.broadcasted_iota(jnp.int32, (256, 256), 1) + chip * 256
    e = (own_maps == spots).astype(BF)

    block = jax.ShapeDtypeStruct((W, ROWS), BF)
    send2, piv, diags = call(forward_children, [sent, block, jax.ShapeDtypeStruct((2, 16, ROWS), BF)], pos, xg, first, first_other, others, others_got, e)
    g2 = exchange(send2)
    second = joined(pos, after(second_x, piv))
    second_other = partner(second)
    send3 = call(parent_forward, sent, pos, g2, second, second_other, diags)
    g3 = exchange(send3)
    part = call(pivot_backward, jax.ShapeDtypeStruct((2, HALF, W), F32), pos, g2, piv, first, first_other)
    send4, sol_t = call(parent_backward, [sent, jax.ShapeDtypeStruct((W, ROWS), F32)], pos, g3, second, second_other, e)
    g4 = exchange(send4)
    s0, s1 = halves(sol_t, core, 1)
    s_got = partner(s1)
    parent_solution = jnp.concatenate(sides(s0, s_got), axis=0).T

    out_half = jax.ShapeDtypeStruct((2, 64, W), F32)
    mine, other = call(children_backward, [out_half, out_half], pos, g4, second, second_other, part)
    got = partner(other)
    child_solution = jnp.concatenate(sides(mine, got), axis=2)
    return (parent_solution, child_solution)


def solution(mesh):
    fine = Mesh(mesh.devices.reshape(2, 8, 2, 4, 4), ("yl", "z", "c", "x", "yh"))
    three = P(None, PANEL, RHS)
    two = P(PANEL, RHS)

    return jax.shard_map(
        shards,
        mesh=fine,
        in_specs=(three, two, two, three, two, two, two, three, three, P()),
        out_specs=(two, three),
        check_vma=False,
    )
```

```python
import jax
import jax.numpy as jnp
from jax import lax
from jax.experimental import pallas as pl
from jax.experimental.pallas import tpu as pltpu
from jax.sharding import Mesh, PartitionSpec as P


BF = jnp.bfloat16
F32 = jnp.float32
CHIPS = ("yl", "z")
RHS = ("x", "yh")
PANEL = ("yl", "z", "c")
NP = 16
W = 64
ROWS = 256
HALF = 128


def nt(a, b):
    return lax.dot_general(a, b, (((1,), (1,)), ((), ())), preferred_element_type=F32)


def nn(a, b):
    return lax.dot_general(a, b, (((1,), (0,)), ((), ())), preferred_element_type=F32)


def vmem():
    return pl.BlockSpec(memory_space=pltpu.VMEM)


def smem():
    return pl.BlockSpec(memory_space=pltpu.SMEM)


def near(x):
    return pltpu.with_memory_space_constraint(x, pltpu.VMEM)


def from_hbm(kernel, outs, pos, *args):
    return plain(kernel, outs, pos, *[pltpu.with_memory_space_constraint(a, pltpu.HBM) for a in args])


def call(kernel, outs, pos, *args):
    return plain(kernel, outs, pos, *[near(a) if a.ndim > 2 else a for a in args])


def plain(kernel, outs, *args):
    return pl.pallas_call(
        kernel,
        out_shape=outs,
        in_specs=[smem()] + [vmem()] * (len(args) - 1),
        out_specs=jax.tree.map(lambda _: vmem(), outs),
        compiler_params=pltpu.CompilerParams(vmem_limit_bytes=16 * 2**20),
    )(*args)


def ordered(both, core):
    half = both.shape[1] // 2
    swapped = jnp.concatenate([both[:, half:], both[:, :half]], axis=1)
    return jnp.where(core == 0, both, swapped)


def row_ids(core, n):
    at = lax.broadcasted_iota(jnp.int32, (n, n), 0)
    half = n // 2
    return jnp.where(core == 0, at, jnp.where(at < half, at + half, at - half))


def keep(x, cond):
    return jnp.where(cond, x, jnp.zeros_like(x))


def pivot_rows(mine, other, at, k):
    cut = slice(k * HALF, (k + 1) * HALF)
    return jnp.concatenate([mine[at, 64:128, cut], other[at, 64:128, cut]], axis=0)


def update_rows(f, at):
    return jnp.concatenate([f[at, 0:64, :HALF], f[at, 0:64, HALF:]], axis=0)


def own_columns(core, rows):
    turned = rows.T
    return jnp.where(core == 0, turned[:W], turned[W:])


def write_terms(x, out, at):
    high = x.astype(BF)
    n = x.shape[0]
    out[at : at + n] = high
    out[at + n : at + 2 * n] = (x - high.astype(F32)).astype(BF)


def ready(pos, pivot_rhs, update_rhs, parent_rhs, lower_update, x_out, moved_out, parent_out):
    x_out[...] = jnp.concatenate([pivot_rhs[0], pivot_rhs[1]], axis=0).astype(BF)
    moved_out[0:HALF] = lower_update[...]
    write_terms(update_rhs[...], moved_out, HALF)
    write_terms(parent_rhs[...], parent_out, 0)


def packed(pos, lower_pivot, upper_pivot, parent_lower, parent_upper, upper_update, first_out, second_out):
    chip, core, group = pos[0], pos[1], pos[36]
    sides = []
    for k in range(2):
        at = lax.broadcasted_iota(jnp.int32, (64, HALF), 0) + core * 64
        to = lax.broadcasted_iota(jnp.int32, (64, HALF), 1)
        lower = lower_pivot[k].astype(F32)
        low = jnp.logical_or(group < chip, jnp.logical_and(group == chip, to < at))
        sides.append(jnp.where(low, lower, upper_pivot[k].astype(F32)))
        on = jnp.logical_and(group == chip, to == at)
        sides.append(jnp.sum(keep(lower, on), axis=0, keepdims=True))
    first_out[0:64] = jnp.concatenate([sides[0], sides[2]], axis=1).astype(BF)
    at = lax.broadcasted_iota(jnp.int32, (HALF, ROWS), 0) + core * HALF
    to = lax.broadcasted_iota(jnp.int32, (HALF, ROWS), 1)
    lower = parent_lower[...].astype(F32)
    low = jnp.logical_or(group < chip, jnp.logical_and(group == chip, to < at))
    second_out[0:HALF] = jnp.where(low, lower, parent_upper[...].astype(F32)).astype(BF)
    on = jnp.logical_and(group == chip, to == at)
    parent_diag = jnp.sum(keep(lower, on), axis=0, keepdims=True)
    pivot_diag = jnp.concatenate([sides[1], sides[3]], axis=1)
    row = lax.broadcasted_iota(jnp.int32, (16, ROWS), 0)
    first_out[64:80] = jnp.where(row == 0, pivot_diag, jnp.where(row == 1, parent_diag, 0.0)).astype(BF)
    second_out[HALF:] = jnp.concatenate([upper_update[0], upper_update[1]], axis=1)


def columns_joined(pos, mine, got, out):
    core = pos[1]
    for k in range(2):
        a, b = mine[k], got[k]
        out[k] = jnp.where(core == 0, jnp.concatenate([a, b], axis=1), jnp.concatenate([b, a], axis=1))


def first_block(pos, mine, other, send):
    core = pos[1]
    a = mine[...].astype(F32)
    b = other[...].astype(F32)
    low, high = jnp.where(core == 0, a, b), jnp.where(core == 0, b, a)
    rows = jnp.concatenate([low[:64], high[:64], low[64:], high[64:]], axis=0)
    block = own_columns(core, rows).astype(BF)
    for q in range(NP):
        send[q] = block


def join(pos, a, b, c, d, out):
    for i, x in enumerate((a, b, c, d)):
        out[4 * i : 4 * i + 4] = x[...]


def joined(pos, pieces):
    n, *rest = pieces[0].shape
    return call(join, jax.ShapeDtypeStruct((4 * n, *rest), pieces[0].dtype), pos, *pieces)


def forward_children(pos, xg, fm, fo, mine, other, e, send, piv_out):
    chip, core, mid_at = pos[0], pos[1], pos[2]
    acc_m = jnp.zeros((W, HALF), F32)
    acc_o = jnp.zeros((W, HALF), F32)
    piv = [jnp.zeros((W, HALF), F32), jnp.zeros((W, HALF), F32)]
    for r in range(NP):
        src = pos[4 + r]
        x = xg[src]
        xs = (x[:, :HALF], x[:, HALF:])
        xc = jnp.where(core == 0, xs[0], xs[1])
        xo = jnp.where(core == 0, xs[1], xs[0])
        acc_m += nt(xc, update_rows(fm, r))
        acc_o += nt(xo, update_rows(fo, r))
        for k in range(2):
            piv[k] += nt(keep(xs[k], src < chip), pivot_rows(fm, fo, r, k))
    terms = [x[...].astype(F32) for x in (mine, other)]
    acc_m += own_columns(core, terms[0][:HALF] + terms[0][HALF : 2 * HALF])
    acc_o += own_columns(core, terms[1][:HALF] + terms[1][HALF : 2 * HALF])
    u0 = jnp.where(core == 0, acc_m, acc_o)
    u1 = jnp.where(core == 0, acc_o, acc_m)
    pr_m, pr_o = (t[2 * HALF : 3 * HALF] + t[3 * HALF :] for t in terms)
    pr_rows = jnp.concatenate([jnp.where(core == 0, pr_m, pr_o), jnp.where(core == 0, pr_o, pr_m)], axis=0)
    pr = own_columns(core, pr_rows)
    u = jnp.concatenate([u0.astype(BF), u1.astype(BF)], axis=1)
    ps = (pr + nn(u, e[...])).astype(BF)
    rows = row_ids(core, HALF)
    cols = lax.broadcasted_iota(jnp.int32, (HALF, HALF), 1)
    own = xg[chip]
    diags = fm[mid_at, 128:144, :].astype(F32) + fo[mid_at, 128:144, :].astype(F32)
    diag = diags[0:1]
    outs = []
    for k in range(2):
        cut = slice(k * HALF, (k + 1) * HALF)
        x = own[:, cut]
        total = ordered(piv[k] + nt(x, keep(pivot_rows(fm, fo, mid_at, k), cols < rows)), core)
        outs.append((total + x.astype(F32) * diag[:, cut]).astype(BF))
    pivot = jnp.concatenate(outs, axis=1)
    piv_out[0:W] = pivot
    piv_out[W:] = diags.astype(BF)
    for q in range(NP):
        send[q] = jnp.where(chip <= q, ps, pivot)


def parent_forward(pos, g, mm, mo, diags, send):
    chip, core, mid_at = pos[0], pos[1], pos[3]
    acc_m = jnp.zeros((W, HALF), F32)
    acc_o = jnp.zeros((W, HALF), F32)
    for r in range(NP):
        src = pos[20 + r]
        x = keep(g[src], src < chip)
        acc_m += nt(x, mm[r, 0:HALF, :])
        acc_o += nt(x, mo[r, 0:HALF, :])
    rows = row_ids(core, ROWS)
    cols = lax.broadcasted_iota(jnp.int32, (ROWS, ROWS), 1)
    block = jnp.concatenate([mm[mid_at, 0:HALF, :], mo[mid_at, 0:HALF, :]], axis=0)
    ps = g[chip]
    total = ordered(jnp.concatenate([acc_m, acc_o], axis=1) + nt(ps, keep(block, cols < rows)), core)
    diag = diags[W : W + 16].astype(F32)[1:2]
    mid = (total + ps.astype(F32) * diag).astype(BF)
    for q in range(NP):
        send[q] = mid


def parent_backward(pos, g, mm, mo, e, send, sol_out):
    chip, core, mid_at = pos[0], pos[1], pos[3]
    acc_m = jnp.zeros((W, HALF), F32)
    acc_o = jnp.zeros((W, HALF), F32)
    for r in range(NP):
        src = pos[20 + r]
        x = keep(g[src], src > chip)
        acc_m += nt(x, mm[r, 0:HALF, :])
        acc_o += nt(x, mo[r, 0:HALF, :])
    rows = row_ids(core, ROWS)
    cols = lax.broadcasted_iota(jnp.int32, (ROWS, ROWS), 1)
    block = jnp.concatenate([mm[mid_at, 0:HALF, :], mo[mid_at, 0:HALF, :]], axis=0)
    sol = ordered(jnp.concatenate([acc_m, acc_o], axis=1) + nt(g[chip], keep(block, cols >= rows)), core)
    sol_out[...] = sol
    picked = nt(sol.astype(BF), e[...]).astype(BF)
    for q in range(NP):
        send[q] = picked


def pivot_backward(pos, g, piv_ref, fm, fo, out):
    chip, core, mid_at = pos[0], pos[1], pos[2]
    rows = row_ids(core, HALF)
    cols = lax.broadcasted_iota(jnp.int32, (HALF, HALF), 1)
    for k in range(2):
        cut = slice(k * HALF, (k + 1) * HALF)
        acc = jnp.zeros((HALF, W), F32)
        for r in range(NP):
            src = pos[4 + r]
            acc += nt(pivot_rows(fm, fo, r, k), keep(g[src, :, cut], src > chip))
        acc += nt(keep(pivot_rows(fm, fo, mid_at, k), cols >= rows), piv_ref[0:W, cut])
        out[k] = acc


def children_backward(pos, g, um, uo, part, mine, other):
    for k in range(2):
        acc = part[k]
        for r in range(NP):
            cut = slice(k * HALF, (k + 1) * HALF)
            block = jnp.concatenate([um[r, 128:192, cut], uo[r, 128:192, cut]], axis=0)
            acc += nt(block, g[pos[20 + r], :, cut])
        mine[k] = acc[:64]
        other[k] = acc[64:]


def to_all(block, axes, n):
    return lax.all_to_all(jnp.broadcast_to(block[None], (n, *block.shape)), axes, 0, 0, tiled=True)


def shifts(x, axis):
    moved = [x]
    for k in (1, 2, 3):
        moved.append(lax.ppermute(x, axis, [(i, (i + k) % 4) for i in range(4)]))
    return moved


def partner(x):
    return lax.ppermute(x, "c", [(0, 1), (1, 0)])


def after(x, *done):
    return lax.optimization_barrier((x, done))[0]


def exchange(send):
    return lax.all_to_all(send, CHIPS, 0, 0, tiled=True)


def halves(x, core, axis):
    a, b = jnp.split(x, 2, axis=axis)
    return jnp.where(core == 0, a, b), jnp.where(core == 0, b, a)


def shards(pivot_rhs, update_rhs, parent_rhs, lower_pivot, lower_update, parent_lower, parent_upper, upper_pivot, upper_update, maps):
    core = lax.axis_index("c")
    chip = lax.axis_index("yl") * 8 + lax.axis_index("z")
    group = lax.axis_index("x") * 4 + lax.axis_index("yh")
    place = jnp.arange(4)
    gx, gy = lax.axis_index("x"), lax.axis_index("yh")
    y_from = (gy - place) % 4
    x_from = (gx - place) % 4
    y_at = (gy - chip % 4) % 4
    sources_ax = (place[:, None] * 4 + y_from[None, :]).reshape(16)
    sources_rx = (x_from[:, None] * 4 + y_from[None, :]).reshape(16)
    mid_ax = chip // 4 * 4 + y_at
    mid_rx = (gx - chip // 4) % 4 * 4 + y_at
    pos = jnp.concatenate([jnp.stack([chip, core, mid_ax, mid_rx]), sources_ax, sources_rx, group[None]]).astype(jnp.int32)

    to_parent = []
    for p in range(32):
        k, j = divmod(p, 16)
        to_parent.append((p, 2 * j + k))
    shapes = [jax.ShapeDtypeStruct((n, 128), BF) for n in (128, 384, 256)]
    x_rows, to_move, parent_terms = from_hbm(ready, shapes, pos, pivot_rhs, update_rhs, parent_rhs, lower_update)
    moved = lax.ppermute(to_move, PANEL, to_parent)

    x_other = partner(x_rows)
    sent = jax.ShapeDtypeStruct((NP, W, ROWS), BF)
    send1 = call(first_block, sent, pos, x_rows, x_other)
    xg = exchange(send1)

    def sides(mine, other):
        return jnp.where(core == 0, mine, other), jnp.where(core == 0, other, mine)

    shapes = [jax.ShapeDtypeStruct((n, 256), BF) for n in (80, 192)]
    pivots, second_own = from_hbm(packed, shapes, pos, lower_pivot, upper_pivot, parent_lower, parent_upper, upper_update)
    first_own = jnp.concatenate([jnp.concatenate([moved[0:64], moved[64:128]], axis=1), pivots], axis=0)
    first_y = shifts(first_own, "yh")
    first_y, xg = lax.optimization_barrier((jnp.stack(first_y), xg))
    first = to_all(first_y, "x", 4).reshape(16, 144, 256)
    first_other = partner(first)
    second_y = jnp.stack(shifts(second_own, "yh"))
    second_x = shifts(second_y, "x")

    others = jnp.concatenate([moved[128:], parent_terms], axis=0)
    others_got = partner(others)

    own_maps = lax.dynamic_slice(maps.reshape(2, 2048), (0, chip * 128), (2, 128)).reshape(256, 1)
    spots = lax.broadcasted_iota(jnp.int32, (256, 256), 1) + chip * 256
    e = (own_maps == spots).astype(BF)

    kept = pltpu.HBM((W + 16, ROWS), BF)
    send2, piv = call(forward_children, [sent, kept], pos, xg, first, first_other, others, others_got, e)
    g2 = exchange(send2)
    second = joined(pos, after(second_x, piv))
    second_other = partner(second)
    send3 = call(parent_forward, sent, pos, g2, second, second_other, piv)
    g3 = exchange(send3)
    part = call(pivot_backward, jax.ShapeDtypeStruct((2, HALF, W), F32), pos, g2, piv, first, first_other)
    send4, sol_t = call(parent_backward, [sent, jax.ShapeDtypeStruct((W, ROWS), F32)], pos, g3, second, second_other, e)
    g4 = exchange(send4)
    s0, s1 = halves(sol_t, core, 1)
    s_got = partner(s1)
    parent_solution = jnp.concatenate(sides(s0, s_got), axis=0).T

    out_half = jax.ShapeDtypeStruct((2, 64, W), F32)
    mine, other = call(children_backward, [out_half, out_half], pos, g4, second, second_other, part)
    got = partner(other)
    child_solution = plain(columns_joined, jax.ShapeDtypeStruct((2, 64, 128), F32), pos, mine, got)
    return (parent_solution, child_solution)


def solution(mesh):
    fine = Mesh(mesh.devices.reshape(2, 8, 2, 4, 4), ("yl", "z", "c", "x", "yh"))
    three = P(None, PANEL, RHS)
    two = P(PANEL, RHS)

    return jax.shard_map(
        shards,
        mesh=fine,
        in_specs=(three, two, two, three, two, two, two, three, three, P()),
        out_specs=(two, three),
        check_vma=False,
    )
```
